32 devices in a mesh: dp: 8 (over z, x), tp: 4 (over y, core).
Axes of the slice: x: 2, y: 2, z: 4, core: 2. Of those that a mesh axis runs over, the one named last changes fastest.
Arguments:
- queries: bfloat16 [512, 73728], P('dp', 'tp'), may hold values from -32 to 32
- prefix_cache: bfloat16 [8, 576, 1024], P('dp', None, 'tp'), may hold values from -12 to 12
- suffix_cache: bfloat16 [512, 576, 128], P('dp'), may hold values from -48 to 48
- w_uv: bfloat16 [128, 512, 128], P('tp'), may hold values from -1 to 1
- fork_prompt: int32 [512, 1], P('dp'), may hold values from 0 to 7; in each aligned block of 64 rows (0 to 63, 64 to 127, ...) at most 16 rows name the same one
- prompt_slot: int32 [8], replicated, may hold values from 0 to 7, each once
- suffix_len: int32 [512], P('dp'), may hold values from 32 to 128
Outputs:
- attended: bfloat16 [512, 16384], P('dp', 'tp')
The draws below stay inside these ranges and needn't reach their ends.
Inputs may be any that keep to these rules, and one draw needn't show every extreme that they name: `fork_prompt`: among the 64 forks of one index of dp no prompt is named more than 16 times. `prompt_slot`: each slot holds exactly one prompt.
All inputs are finite; a program needn't handle non-finite values.
Results may differ from the reference program's by a relative error of at most 0.033.
Values may be sent and summed in bfloat16 or wider, within the bound.
A program may use at most 128 MiB of HBM per device.

```python
import math
import jax
import jax.numpy as jnp
import numpy as np
from jax import lax

H = 128
R = 512
P_SIZE = 64
V = 128
L = 1024
S = 128
FORK_DEV = 64
MOST = 16
PROMPTS = 8
FORKS = 512


def fork_pair(key):
    base = jax.random.fold_in(key, 7001)
    streams = jax.random.split(base, 2)
    key_width = R + P_SIZE
    suffix = jnp.clip(jax.random.normal(streams[0], (FORKS, key_width, S), jnp.float32), -4.0, 4.0)
    query = jnp.clip(jax.random.normal(streams[1], (FORKS, H, key_width), jnp.float32), -4.0, 4.0)
    suffix = jnp.clip(suffix, -48.0, 48.0)
    query = jnp.clip(query, -32.0, 32.0)
    return (query, suffix)


def draw_queries(key, part):
    query, suffix = fork_pair(key)
    return query.reshape(FORKS, H * (R + P_SIZE)).astype(jnp.bfloat16)


def draw_suffix_cache(key, part):
    query, suffix = fork_pair(key)
    return suffix.astype(jnp.bfloat16)


def draw_prefix_cache(key, part):
    base = jax.random.fold_in(key, 7002)
    streams = jax.random.split(base, 1)
    cache = jnp.clip(jax.random.normal(streams[0], (PROMPTS, R + P_SIZE, L), jnp.float32), -4.0, 4.0)
    return cache.astype(jnp.bfloat16)


def set_ends(values, key, low, high):
    longest = values.shape.index(max(values.shape))
    spots = []
    for shift in (0, 1):
        where = [jax.random.randint(jax.random.fold_in(key, axis), (), 0, length) for axis, length in enumerate(values.shape)]
        where[longest] = (where[longest] + shift) % values.shape[longest]
        spots.append(tuple(where))
    return values.at[spots[0]].set(low).at[spots[1]].set(high)


def shard_levels(stream_key, shape, shards, low, high):
    def one(axis_at, parts):
        steps = jax.random.uniform(jax.random.fold_in(jax.random.fold_in(stream_key, 6), axis_at), (parts,), jnp.float32, low / len(shards), high / len(shards))
        return jnp.repeat(jnp.exp(steps), shape[axis_at] // parts).reshape((-1,) + (1,) * (len(shape) - axis_at - 1))

    level = one(*shards[0])
    for cut in shards[1:]:
        level = level * one(*cut)
    return level


def shared_out(rng, own, number, rows, number_of, top, bound, skew):
    sequence = jax.random.permutation(rng, number_of)
    packed, common = portions_of(number_of, rows * top, bound, skew, True), portions_of(number_of, rows * top, bound, skew, False)
    places = jnp.arange(number_of)

    def named(lengths, rotation):
        used = int((lengths > 0).sum())
        fixed = max(1, used // 4)
        moved = fixed + (places - fixed + rotation * (used - fixed)) % max(1, number_of - fixed)
        return jnp.zeros((number_of,), jnp.int32).at[sequence[jnp.where(places < fixed, places, moved)]].set(jnp.asarray(lengths, jnp.int32))

    lengths = jnp.where(number % 4 == 0, named(packed, number // 4), named(common, number - number // 4 - 1))
    mixed = jax.random.permutation(jax.random.fold_in(own, 3), number_of)
    source_of, sink = mixed[0:number_of // 2 * 2:2], mixed[1:number_of // 2 * 2:2]
    slack = jnp.minimum(lengths[source_of] - 1, bound - lengths[sink]) // 2
    slack = jnp.where((source_of == sequence[0]) | (sink == sequence[0]) | (lengths[sink] == 0), 0, jnp.maximum(slack, 0))
    moved = jax.random.randint(jax.random.fold_in(own, 4), (number_of // 2,), 0, 1 << 20) % (slack + 1)
    lengths = lengths.at[source_of].add(-moved).at[sink].add(moved)
    members = jnp.searchsorted(jnp.cumsum(lengths), jnp.arange(rows * top), side="right").astype(jnp.int32)
    table = members.reshape(top, rows).T
    table = table[jax.random.permutation(jax.random.fold_in(own, 1), rows)]
    rotation = jax.random.randint(jax.random.fold_in(own, 2), (rows, 1), 0, top)
    return jnp.take_along_axis(table, (jnp.arange(top)[None, :] + rotation) % top, axis=1)


def portions_of(amount, total, bound, slope, full):
    weights = [(1 << 20) // math.isqrt(standing ** slope) + 1 for standing in range(1, amount + 1)]
    largest = bound if full else min(bound, max(-(-total // amount), total * weights[0] // sum(weights)))
    least = 1 if total - largest >= amount - 1 else 0
    counts, rest = [largest] + [least] * (amount - 1), total - largest - least * (amount - 1)
    while rest > 0:
        movable = [i for i in range(1, amount) if counts[i] < largest] or [i for i in range(1, amount) if counts[i] < bound]
        pool, budget = sum([weights[i] for i in movable]), rest
        for i in movable:
            more = min(bound - counts[i], max(1, budget * weights[i] // pool), rest)
            counts[i] = counts[i] + more
            rest = rest - more
    return np.array(counts)


def normal_values(own_key, dims, scale, most, pieces=(), kind=jnp.bfloat16):
    values = scale * jax.random.normal(own_key, dims, jnp.float32)
    if pieces:
        values = values * shard_levels(own_key, dims, pieces, -0.22, 0.18)
    return jnp.clip(values, -most, most).astype(kind)


def setup_inputs(seed: int = 0) -> dict:
    arg_keys = jax.random.split(jax.random.key(seed), 8)
    queries = draw_queries(jax.random.fold_in(arg_keys[7], 71), 0)
    prefix_cache = draw_prefix_cache(jax.random.fold_in(arg_keys[7], 71), 0)
    suffix_cache = draw_suffix_cache(jax.random.fold_in(arg_keys[7], 71), 0)
    w_uv = normal_values(arg_keys[3], (H, R, V), (R // 16) ** -0.5, 1.0, ((0, 4),))
    fork_prompt_keys = jax.random.split(jax.random.fold_in(arg_keys[4], 1), FORKS // FORK_DEV)
    fork_prompt_turns = jax.random.permutation(jax.random.fold_in(arg_keys[4], 3), FORKS // FORK_DEV)
    fork_prompt = jax.vmap(lambda own, number: shared_out(jax.random.fold_in(arg_keys[4], 2), own, number, FORK_DEV, PROMPTS, 1, MOST, 2))(fork_prompt_keys, fork_prompt_turns).reshape((FORKS, 1))
    prompt_slot = jax.random.permutation(arg_keys[5], PROMPTS).astype(jnp.int32)
    suffix_len = set_ends(jax.random.randint(arg_keys[6], (FORKS,), S // 4, S + 1), jax.random.fold_in(arg_keys[6], 1), S // 4, S).astype(jnp.int32)
    return {"queries": queries, "prefix_cache": prefix_cache, "suffix_cache": suffix_cache, "w_uv": w_uv, "fork_prompt": fork_prompt, "prompt_slot": prompt_slot, "suffix_len": suffix_len}


score_scale = 192.0 ** -0.5


def attend(query_heads, keys, live_mask):
    scores = jnp.einsum('bhe,bek->bhk', query_heads, keys) * score_scale
    scores = jnp.where(live_mask, scores, -jnp.inf)
    peak = jnp.max(scores, axis=2, keepdims=True)
    weights = jnp.where(live_mask, jnp.exp(scores - peak), 0.0)
    mass_sum = jnp.sum(weights, axis=2)
    rounded = lax.optimization_barrier(weights.astype(jnp.bfloat16)).astype(jnp.float32)
    summed = jnp.einsum('bhk,brk->bhr', rounded, keys[:, :R, :])
    latent = (summed / mass_sum[..., None]).astype(jnp.bfloat16)
    return latent, peak[..., 0] + jnp.log(mass_sum)


def project(latent, w_full):
    return jnp.einsum('bhr,hrv->bhv', latent.astype(jnp.float32), w_full).astype(jnp.bfloat16)


def reference(queries, prefix_cache, suffix_cache, w_uv, fork_prompt, prompt_slot, suffix_len):
    owner_slot = jnp.take(prompt_slot, fork_prompt[:, 0]).astype(jnp.int32)
    blocks = FORKS // FORK_DEV
    w_full = w_uv.astype(jnp.float32)

    def one_block(items):
        block_queries, block_suffix, block_owner, block_lengths = items
        query_heads = block_queries.astype(jnp.float32).reshape(FORK_DEV, H, R + P_SIZE)
        prefix_keys = jnp.take(prefix_cache, block_owner, axis=0).astype(jnp.float32)
        all_live = jnp.ones((FORK_DEV, 1, L), dtype=bool)
        latent_prefix, mass_prefix = attend(query_heads, prefix_keys, all_live)
        positions = jnp.arange(S).astype(jnp.int32)
        suffix_live = (positions[None, :] < block_lengths[:, None])[:, None, :]
        latent_suffix, mass_suffix = attend(query_heads, block_suffix.astype(jnp.float32), suffix_live)
        value_prefix = project(latent_prefix, w_full).astype(jnp.float32)
        value_suffix = project(latent_suffix, w_full).astype(jnp.float32)
        top_mass = jnp.maximum(mass_prefix, mass_suffix)
        share_prefix = jnp.exp(mass_prefix - top_mass)[..., None]
        share_suffix = jnp.exp(mass_suffix - top_mass)[..., None]
        combined = (share_prefix * value_prefix + share_suffix * value_suffix) / (share_prefix + share_suffix)
        return combined.astype(jnp.bfloat16).reshape(FORK_DEV, H * V)

    result = lax.map(one_block, (queries.reshape(blocks, FORK_DEV, H * (R + P_SIZE)),
                                 suffix_cache.reshape(blocks, FORK_DEV, R + P_SIZE, S),
                                 owner_slot.reshape(blocks, FORK_DEV),
                                 suffix_len.reshape(blocks, FORK_DEV)))
    return result.reshape(FORKS, H * V)
```

```python
import functools

import jax
import jax.numpy as jnp
from jax import lax
from jax.experimental import pallas as pl
from jax.experimental.pallas import tpu as pltpu
from jax.sharding import PartitionSpec as P

R = 512
P_SIZE = 64
V = 128


score_scale = 192.0 ** (-0.5)
log2e = 1.4426950408889634
OUTER = (((1,), (1,)), ((), ()))


def project(latent, w_uv):
    return jnp.einsum("nhr,hrv->nhv", latent, w_uv, preferred_element_type=jnp.float32).astype(
        jnp.bfloat16
    )


def exchange_plan(queries, prefix_cache, suffix_cache, w_uv, fork_prompt, prompt_slot, suffix_len):
    owners_count = lax.axis_size("dp")
    forks_here = queries.shape[0]
    heads_here = w_uv.shape[0]
    key_width = R + P_SIZE
    capacity = max(2, 2 * forks_here // owners_count)
    slots_all = owners_count * capacity
    prompt_ids = jnp.arange(prompt_slot.shape[0], dtype=jnp.int32)
    chosen = fork_prompt[:, 0][:, None] == prompt_ids[None, :]
    owner_slot = jnp.sum(jnp.where(chosen, prompt_slot[None, :], 0), axis=1)
    fork_order = jnp.arange(forks_here, dtype=jnp.int32)
    before = (owner_slot[:, None] == owner_slot[None, :]) & (
        fork_order[None, :] < fork_order[:, None]
    )
    slot_rank = jnp.sum(before.astype(jnp.int32), axis=1)
    target = owner_slot * capacity + slot_rank
    placing = target[None, :] == jnp.arange(slots_all, dtype=jnp.int32)[:, None]
    outbound = jnp.dot(
        placing.astype(jnp.bfloat16), queries, preferred_element_type=jnp.float32
    ).astype(jnp.bfloat16)
    outbound = outbound.reshape(owners_count, capacity, heads_here * key_width)
    gathered = lax.all_gather(prefix_cache, "tp", axis=2, tiled=True)[0]
    received = lax.all_to_all(outbound, "dp", split_axis=0, concat_axis=0, tiled=True)
    sources = received.shape[0]
    items = received.shape[1]
    lead_rows = sources * items
    query_rows = received.reshape(lead_rows * heads_here, key_width)
    scores = jnp.dot(query_rows, gathered, preferred_element_type=jnp.float32) * score_scale
    peak_score = jnp.max(scores, axis=1, keepdims=True)
    weights = jnp.exp(scores - peak_score)
    mass_sum = jnp.sum(weights, axis=1)
    summed = lax.dot_general(
        weights.astype(jnp.bfloat16),
        gathered[:R],
        (((1,), (1,)), ((), ())),
        preferred_element_type=jnp.float32,
    )
    latent = (summed / mass_sum[:, None]).astype(jnp.bfloat16)
    log_mass = (peak_score[:, 0] + jnp.log(mass_sum)).reshape(sources, items, heads_here)
    result = project(latent.reshape(lead_rows, heads_here, R), w_uv)
    result = result.reshape(sources, items, heads_here * V)
    answer, answer_mass = (
        lax.all_to_all(result, "dp", split_axis=0, concat_axis=0, tiled=True),
        lax.all_to_all(
            log_mass.astype(jnp.bfloat16), "dp", split_axis=0, concat_axis=0, tiled=True
        ).astype(log_mass.dtype),
    )
    picking = placing.astype(jnp.bfloat16)
    flat_answer = answer.reshape(slots_all, answer.shape[2])
    returned = lax.dot_general(
        picking, flat_answer, (((0,), (0,)), ((), ())), preferred_element_type=jnp.float32
    ).astype(jnp.bfloat16)
    mass_prefix = lax.dot_general(
        placing.astype(jnp.float32),
        answer_mass.reshape(slots_all, heads_here),
        (((0,), (0,)), ((), ())),
        precision=lax.Precision.HIGHEST,
    )
    value_prefix = returned.reshape(forks_here, heads_here, V)
    query_heads = queries.reshape(forks_here, heads_here, key_width)
    suffix_scores = (
        jnp.einsum("fhe,fes->fhs", query_heads, suffix_cache, preferred_element_type=jnp.float32)
        * score_scale
    )
    positions = jnp.arange(suffix_cache.shape[2], dtype=jnp.int32)
    live_mask = (positions[None, :] < suffix_len[:, None])[:, None, :]
    suffix_scores = jnp.where(live_mask, suffix_scores, -jnp.inf)
    suffix_peak = jnp.max(suffix_scores, axis=2, keepdims=True)
    suffix_weights = jnp.where(live_mask, jnp.exp(suffix_scores - suffix_peak), 0.0)
    suffix_sum = jnp.sum(suffix_weights, axis=2)
    suffix_summed = jnp.einsum(
        "fhs,frs->fhr",
        suffix_weights.astype(jnp.bfloat16),
        suffix_cache[:, :R, :],
        preferred_element_type=jnp.float32,
    )
    latent_suffix = (suffix_summed / suffix_sum[..., None]).astype(jnp.bfloat16)
    mass_suffix = suffix_peak[..., 0] + jnp.log(suffix_sum)
    value_suffix = project(latent_suffix, w_uv)
    top_mass = jnp.maximum(mass_prefix, mass_suffix)
    share_prefix = jnp.exp(mass_prefix - top_mass)[..., None]
    share_suffix = jnp.exp(mass_suffix - top_mass)[..., None]
    combined = (
        share_prefix * value_prefix.astype(jnp.float32)
        + share_suffix * value_suffix.astype(jnp.float32)
    ) / (share_prefix + share_suffix)
    return combined.astype(jnp.bfloat16).reshape(forks_here, heads_here * V)


MESH = pl.DeviceIdType.MESH
PAIR = 2 * (R + P_SIZE)
WINDOW = R + 2 * P_SIZE
TILES = WINDOW // 128
PITCH = 2 * TILES + 1


def slot_rows(owner, prompts, capacity):
    forks = owner.shape[0]
    wide = jnp.broadcast_to(owner, (forks, forks)).astype(jnp.float32)
    down = lax.broadcasted_iota(jnp.int32, (forks, forks), 0)
    across = lax.broadcasted_iota(jnp.int32, (forks, forks), 1)
    owner_row = jnp.sum(jnp.where(down == across, wide, 0.0), axis=0, keepdims=True)
    ahead = (wide == owner_row) & (down < across)
    rank = jnp.sum(jnp.where(ahead, 1.0, 0.0), axis=0, keepdims=True)
    target = (owner_row * capacity + rank).astype(jnp.int32)
    rows = lax.broadcasted_iota(jnp.int32, (prompts * capacity, forks), 0)
    return jnp.where(rows == target, 1.0, 0.0)


def stage_queries(p, q_ref, perm, staged_ref, sorted_ref):
    forks = q_ref.shape[0]
    columns = pl.ds(pl.multiple_of(p * PAIR, 128), PAIR)
    pair = q_ref[:, columns]
    sorted_ref[p] = jnp.dot(perm, pair, preferred_element_type=jnp.float32).astype(jnp.bfloat16)
    pair = pair.astype(jnp.float32)
    even = pair[:, :WINDOW]
    odd = pltpu.roll(pair[:, PAIR - WINDOW :], WINDOW - P_SIZE, 1)
    pairs = sorted_ref.shape[0]
    for b in range(forks // 8):
        for j in range(TILES):
            for half, part in enumerate((even, odd)):
                row = ((b * pairs + p) * PITCH + half * TILES + j) * 8
                staged_ref[pl.ds(pl.multiple_of(row, 8), 8), :] = part[
                    b * 8 : b * 8 + 8, j * 128 : j * 128 + 128
                ]


def suffix_chunk(first, block, pairs, lens_ref, staged_ref, cache_ref, lat_ref, mass_ref):
    width = R + P_SIZE
    heads = 2 * pairs
    pitch = heads + 8
    base = first // 8 * pairs * PITCH * 8 + first % 8
    for s in range(block):
        f = first + s
        halves = []
        for half in range(2):
            halves.append(
                jnp.concatenate(
                    [
                        staged_ref[
                            pl.ds(base + (half * TILES + j) * 8 + s, pairs, stride=PITCH * 8), :
                        ]
                        for j in range(TILES)
                    ],
                    axis=1,
                )
            )
        q = jnp.concatenate(halves, axis=0)[:, :width].astype(jnp.bfloat16)
        positions = lax.broadcasted_iota(jnp.int32, (1, cache_ref.shape[2]), 1)
        live = positions < lens_ref[f]
        scores = jnp.dot(q, cache_ref[f], preferred_element_type=jnp.float32)
        scores = jnp.where(live, scores * (score_scale * log2e), -jnp.inf)
        peak = jnp.max(scores, axis=1, keepdims=True)
        weights = jnp.exp2(scores - peak)
        mass = jnp.sum(weights, axis=1, keepdims=True)
        summed = lax.dot_general(
            weights.astype(jnp.bfloat16),
            cache_ref[f, :R, :],
            OUTER,
            preferred_element_type=jnp.float32,
        )
        latent = summed / mass
        rows = pl.ds(pl.multiple_of(f * pitch, 8), heads)
        for j in range(R // 128):
            lat_ref[j, rows, :] = latent[:, j * 128 : j * 128 + 128]
        mass_ref[rows, :] = jnp.broadcast_to(peak + jnp.log2(mass), (heads, 128))


def exact_rows(perm, value):
    high = value.astype(jnp.bfloat16)
    rest = value - high.astype(jnp.float32)
    mid = rest.astype(jnp.bfloat16)
    low = (rest - mid.astype(jnp.float32)).astype(jnp.bfloat16)
    moved = jnp.dot(
        perm, jnp.concatenate([high, mid, low], axis=1), preferred_element_type=jnp.float32
    )
    n = value.shape[1]
    return moved[:, :n] + moved[:, n : 2 * n] + moved[:, 2 * n :]


def head_of(r, pairs):
    return 2 * (r % pairs) + r // pairs


def suffix_values(r, forks, pairs, perm, lat_ref, mass_ref, w_ref, value_ref, moved_ref):
    pitch = 2 * pairs + 8
    rows = pl.ds(r, forks, stride=pitch)
    latent = jnp.concatenate([lat_ref[j, rows, :] for j in range(R // 128)], axis=1)
    value = jnp.dot(
        latent.astype(jnp.bfloat16), w_ref[head_of(r, pairs)], preferred_element_type=jnp.float32
    ).astype(jnp.bfloat16)
    value_ref[r] = jnp.dot(perm, value, preferred_element_type=jnp.float32).astype(jnp.bfloat16)
    moved_ref[r] = exact_rows(perm, mass_ref[rows, :])


def slot_attention(slot, capacity, sorted_ref, caches_ref, lat_ref, mass_ref):
    pairs = sorted_ref.shape[0]
    parts = caches_ref.shape[1]
    own = pl.ds(pl.multiple_of(slot * capacity, capacity), capacity)
    weights, masses, peaks = [], [], []
    for odd in range(2):
        first = odd * (PAIR - WINDOW)
        q = jnp.concatenate([sorted_ref[p, own, first : first + WINDOW] for p in range(pairs)], axis=0)
        keys = pl.ds((1 - odd) * P_SIZE, WINDOW)
        scores = [
            jnp.dot(q, caches_ref[slot, k, keys, :], preferred_element_type=jnp.float32)
            for k in range(parts)
        ]
        peak = functools.reduce(
            jnp.maximum, [jnp.max(piece, axis=1, keepdims=True) for piece in scores]
        )
        mass = 0.0
        pieces = []
        for k in range(parts):
            weight = jnp.exp2((scores[k] - peak) * (score_scale * log2e))
            mass = mass + jnp.sum(weight, axis=1, keepdims=True)
            pieces.append(weight.astype(jnp.bfloat16))
        weights.append(pieces)
        masses.append(mass)
        peaks.append(peak)
    summed = 0.0
    for k in range(parts):
        summed = summed + lax.dot_general(
            jnp.concatenate([weights[0][k], weights[1][k]], axis=0),
            caches_ref[slot, k, pl.ds(P_SIZE, R), :],
            OUTER,
            preferred_element_type=jnp.float32,
        )
    mass = jnp.concatenate(masses, axis=0)
    peak = jnp.concatenate(peaks, axis=0)
    latent = (summed / mass).astype(jnp.bfloat16)
    lat_ref[:, own, :] = latent.reshape(2 * pairs, capacity, R)
    log_mass = peak * (score_scale * log2e) + jnp.log2(mass)
    mass_ref[:, own, :] = jnp.broadcast_to(log_mass, (log_mass.shape[0], 128)).reshape(
        2 * pairs, capacity, 128
    )


def combine(r, pairs, lat_ref, w_ref, mass_ref, value_ref, moved_ref, out_ref):
    h = head_of(r, pairs)
    value = jnp.dot(lat_ref[r], w_ref[h], preferred_element_type=jnp.float32)
    value = value.astype(jnp.bfloat16).astype(jnp.float32)
    ours, theirs = mass_ref[r], moved_ref[r]
    top = jnp.maximum(ours, theirs)
    ours = jnp.exp2(ours - top)
    theirs = jnp.exp2(theirs - top)
    mixed = (ours * value + theirs * value_ref[r].astype(jnp.float32)) / (ours + theirs)
    out_ref[:, pl.ds(pl.multiple_of(h * 128, 128), 128)] = mixed.astype(jnp.bfloat16)


class Exchange:
    def __init__(self, caches, own, own_sem, sems):
        dp, tp = lax.axis_index("dp"), lax.axis_index("tp")
        self.planes = caches.shape[0] // 2
        self.z, self.x = dp // 2, dp % 2
        self.y, self.c = tp // 2, tp % 2
        self.caches, self.own, self.own_sem = caches, own, own_sem
        self.sems = sems
        self.low = self.z < self.planes // 2
        inward = jnp.where(self.low, self.z + 1, self.z - 1)
        outward = jnp.clip(jnp.where(self.low, self.z - 1, self.z + 1), 0, self.planes - 1)
        self.edge = (self.z == 0) | (self.z == self.planes - 1)
        self.to = dict(
            x=(self.z * 2 + 1 - self.x, tp),
            y=(dp, (1 - self.y) * 2 + self.c),
            pair=(dp, self.y * 2 + 1 - self.c),
            inward=(inward * 2 + self.x, tp),
            outward=(outward * 2 + self.x, tp),
        )
        self.rows = own.shape[1]
        self.pad = (caches.shape[2] - self.rows) // 2

    def plane(self, q):
        return jnp.where(self.low, q, self.planes - 1 - q)

    def place(self, q, far_x=0, far_y=0, half=None):
        xx = 1 - self.x if far_x else self.x
        yy = 1 - self.y if far_y else self.y
        first, count = self.pad, self.rows
        if half is not None:
            count = self.rows // 2
            first = first + half * count
        return self.caches.at[self.plane(q) * 2 + xx, yy * 2 + self.c, pl.ds(first, count)]

    def copy(self, kind, q, half, sender):
        far_x, far_y, index = {
            "u": (0, 0, 0),
            "d": (1, 1, 1),
            "x": (0, 0, 2),
            "y": (0, 0, 3),
            "dx": (0, 1, 4),
            "dy": (1, 0, 4),
        }[kind]
        link = {"x": "x", "dx": "x", "y": "y", "dy": "y"}.get(kind, sender)
        sends = {"inward": 0, "outward": 2, "x": 4, "y": 5, "dx": 6, "dy": 6}
        send = sends[sender] + (kind == "d") if kind in ("u", "d") else sends[kind]
        part = self.place(q, far_x, far_y, half)
        zz = self.plane(q)
        send_sem, recv_sem = self.sems["send"], self.sems["recv"]
        return pltpu.make_async_remote_copy(
            src_ref=part,
            dst_ref=part,
            send_sem=send_sem.at[send, zz, half],
            recv_sem=recv_sem.at[index, zz, half],
            device_id=self.to[link],
            device_id_type=MESH,
        )

    def send(self, kind, q, half, sender=None):
        self.copy(kind, q, half, sender).start()
        self.sent.append((kind, q, half, sender))

    def got(self, kind, q, half):
        self.copy(kind, q, half, "inward").wait_recv()

    def pair(self, q, far_x, far_y):
        part = self.place(q, far_x, far_y)
        xx = 1 - self.x if far_x else self.x
        yy = 1 - self.y if far_y else self.y
        k = (self.plane(q) * 2 + xx) * 2 + yy
        return pltpu.make_async_remote_copy(
            src_ref=part,
            dst_ref=part,
            send_sem=self.sems["pair_send"].at[k],
            recv_sem=self.sems["pair_recv"].at[k],
            device_id=self.to["pair"],
            device_id_type=MESH,
        )

    def load(self):
        return pltpu.make_async_copy(self.own.at[0], self.place_own(), self.own_sem)

    def place_own(self):
        slot = self.z * 2 + self.x
        return self.caches.at[slot, self.y * 2 + self.c, pl.ds(self.pad, self.rows)]

    def barrier(self):
        sem = pltpu.get_barrier_semaphore()
        for name in ("x", "y", "pair", "inward"):
            pl.semaphore_signal(sem, inc=1, device_id=self.to[name], device_id_type=MESH)

        @pl.when(~self.edge)
        def _():
            pl.semaphore_signal(sem, inc=1, device_id=self.to["outward"], device_id_type=MESH)

        pl.semaphore_wait(sem, jnp.where(self.edge, 4, 5))

    def rounds(self, edge):
        send, got = self.send, self.got
        self.sent = []

        def first():
            q = 0 if edge else 1
            for half in range(2):
                send("u", q, half, "inward")
                if not edge:
                    send("u", q, half, "outward")
                send("x", q, half)
                send("y", q, 1 - half)
            self.pair(q, 0, 0).start()

        def both(kind, q):
            got(kind, q, 0)
            got(kind, q, 1)

        def sides(q):
            both("x", q)
            self.pair(q, 1, 0).start()
            both("y", q)
            self.pair(q, 0, 1).start()

        def sides_late(q):
            got("x", q, 1)
            self.pair(q, 1, 0).start()
            got("y", q, 0)
            self.pair(q, 0, 1).start()

        def cross(q):
            got("x", q, 0)
            send("dy", q, 0)
            got("y", q, 1)
            send("dx", q, 1)

        def crossed(q):
            got("dy", q, 0)
            got("dx", q, 1)
            self.pair(q, 1, 1).start()

        def diagonal(q):
            both("d", q)
            self.pair(q, 1, 1).start()

        def e1():
            cross(0)
            got("u", 1, 0)
            send("x", 1, 0)
            send("y", 1, 0)

        def e2():
            got("u", 1, 1)
            send("x", 1, 1)
            send("y", 1, 1)
            self.pair(1, 0, 0).start()
            sides_late(0)

        def e3():
            crossed(0)
            got("u", 2, 0)
            send("x", 2, 0)
            send("y", 2, 0)

        def e4():
            got("u", 2, 1)
            send("x", 2, 1)
            send("y", 2, 1)
            self.pair(2, 0, 0).start()

        def e5():
            sides(1)
            got("u", 3, 0)
            send("x", 3, 0)

        def e6():
            got("u", 3, 1)
            send("y", 3, 1)
            send("y", 3, 0)
            send("x", 3, 1)
            self.pair(3, 0, 0).start()

        def e7():
            sides(2)

        def e8():
            cross(3)
            diagonal(1)

        def e9():
            sides_late(3)

        def e10():
            crossed(3)
            diagonal(2)

        def i1():
            cross(1)
            got("u", 2, 0)
            send("u", 2, 0, "outward")
            got("u", 0, 0)
            send("u", 0, 0, "inward")
            send("x", 0, 0)

        def i2():
            got("u", 2, 1)
            send("u", 2, 1, "outward")
            got("u", 0, 1)
            send("u", 0, 1, "inward")
            send("y", 0, 1)
            send("y", 0, 0)
            send("x", 0, 1)
            self.pair(2, 0, 0).start()
            self.pair(0, 0, 0).start()
            sides_late(1)

        def i3():
            crossed(1)
            for half in range(2):
                send("d", 1, half, "inward")
            got("u", 3, 0)
            send("u", 3, 0, "outward")

        def i4():
            got("u", 3, 1)
            send("u", 3, 1, "outward")
            self.pair(3, 0, 0).start()
            for half in range(2):
                send("d", 1, half, "outward")
            cross(0)
            for q in (2, 3):
                for half in range(2):
                    send("x", q, half)
                    send("y", q, half)

        def i5():
            sides_late(0)

        def i6():
            crossed(0)
            for half in range(2):
                send("d", 0, half, "inward")
            for half in range(2):
                got("d", 2, half)
                send("d", 2, half, "outward")
            self.pair(2, 1, 1).start()

        def i7():
            pass

        def i8():
            sides(2)

        def i9():
            diagonal(3)

        def i10():
            sides(3)

        if edge:
            return [first, e1, e2, e3, e4, e5, e6, e7, e8, e9, e10]
        return [first, i1, i2, i3, i4, i5, i6, i7, i8, i9, i10]

    def round(self, r):
        edge = []
        for side, when in ((True, self.edge), (False, ~self.edge)):
            @pl.when(when)
            def _(side=side):
                self.rounds(side)[r]()
            edge.append(self.sent)
        self.all_sent = getattr(self, "all_sent", [])
        self.all_sent.append(edge)

    def finish(self):
        for side, when in ((0, self.edge), (1, ~self.edge)):
            @pl.when(when)
            def _(side=side):
                for sent in self.all_sent:
                    for item in sent[side]:
                        self.copy(*item).wait_send()
        for k in range(2 * self.caches.shape[0]):
            pltpu.make_async_remote_copy(
                src_ref=self.place_own(), dst_ref=self.place_own(),
                send_sem=self.sems["pair_send"].at[k], recv_sem=self.sems["pair_recv"].at[k],
                device_id=self.to["pair"], device_id_type=MESH).wait_send()

    def pair_done(self, slot, y):
        pltpu.make_async_remote_copy(
            src_ref=self.place_own(), dst_ref=self.place_own(),
            send_sem=self.sems["pair_send"].at[slot * 2 + y], recv_sem=self.sems["pair_recv"].at[slot * 2 + y],
            device_id=self.to["pair"], device_id_type=MESH).wait_recv()


def pick(table, index):
    value = table[-1]
    for i in range(len(table) - 2, -1, -1):
        value = jnp.where(index == i, table[i], value)
    return value


EDGE_SLOTS = ((0, 0), (0, 1), (1, 0), (2, 0), (1, 1), (3, 0), (2, 1), (3, 1))
INNER_SLOTS = ((1, 0), (1, 1), (0, 0), (0, 1), (2, 0), (2, 1), (3, 0), (3, 1))
PLAN = ("hh", "hhh", "hhh", "ah", "ahh", "hah", "hhh", "avvv", "avvv", "avv", "aa")


def fused_kernel(
    slot_ref,
    lens_ref,
    prompt_ref,
    own,
    q_hbm,
    suffix_hbm,
    w_hbm,
    out_ref,
    perm_ref,
    caches,
    held,
    q_ref,
    staged,
    placed,
    w_ref,
    suffix_lat,
    suffix_mass,
    suffix_value,
    moved_mass,
    lat,
    mass,
    load_sems,
    own_sem,
    send_sems,
    recv_sems,
    pair_send,
    pair_recv,
):
    forks = q_ref.shape[0]
    pairs = placed.shape[0]
    slots = caches.shape[0]
    capacity = placed.shape[1] // slots
    exchange = Exchange(
        caches,
        own,
        own_sem,
        dict(send=send_sems, recv=recv_sems, pair_send=pair_send, pair_recv=pair_recv),
    )
    exchange.load().start()
    sources = ((q_hbm, q_ref), (suffix_hbm, held), (w_hbm, w_ref))
    loads = [pltpu.make_async_copy(a, b, load_sems.at[i]) for i, (a, b) in enumerate(sources)]
    loads[0].start()
    exchange.barrier()
    exchange.load().wait()
    exchange.round(0)
    loads[1].start()
    loads[2].start()

    pad = jnp.zeros((caches.shape[1], P_SIZE, caches.shape[3]), jnp.bfloat16)

    def clear(s, carry):
        caches[s, :, :P_SIZE, :] = pad
        caches[s, :, P_SIZE + R + P_SIZE :, :] = pad
        return carry

    lax.fori_loop(0, slots, clear, 0)
    owner = jnp.zeros(prompt_ref.shape, jnp.int32)
    for p in range(slot_ref.shape[0]):
        owner = jnp.where(prompt_ref[...] == p, slot_ref[p], owner)
    perm_ref[...] = slot_rows(owner, slots, capacity).astype(jnp.bfloat16)
    loads[0].wait()

    def stage(p, carry):
        stage_queries(p, q_ref, perm_ref[...], staged, placed)
        return carry

    lax.fori_loop(0, pairs, stage, 0)
    loads[1].wait()
    loads[2].wait()

    kinds = "".join(PLAN)
    count = {kind: kinds.count(kind) for kind in "hav"}
    before = {
        kind: [kinds[:k].count(kind) for k in range(len(kinds))] for kind in "hav"
    }
    starts = [sum(len(part) for part in PLAN[:r]) for r in range(len(PLAN))]
    block = forks // count["h"]
    group = 2 * pairs // count["v"]

    def is_kind(k, kind):
        hit = k < 0
        for i, name in enumerate(kinds):
            if name == kind:
                hit = hit | (k == i)
        return hit

    def step(k, carry):
        for r in range(1, len(PLAN)):
            @pl.when(k == starts[r])
            def _(r=r):
                exchange.round(r)

        @pl.when(is_kind(k, "h"))
        def _():
            first = pick(before["h"], k) * block
            suffix_chunk(first, block, pairs, lens_ref, staged, held, suffix_lat, suffix_mass)

        @pl.when(is_kind(k, "a"))
        def _():
            n = pick(before["a"], k)
            q = jnp.where(
                exchange.edge, pick([s[0] for s in EDGE_SLOTS], n), pick([s[0] for s in INNER_SLOTS], n)
            )
            far = jnp.where(
                exchange.edge, pick([s[1] for s in EDGE_SLOTS], n), pick([s[1] for s in INNER_SLOTS], n)
            )
            xx = jnp.where(far == 1, 1 - exchange.x, exchange.x)
            slot = exchange.plane(q) * 2 + xx
            exchange.pair_done(slot, 0)
            exchange.pair_done(slot, 1)
            slot_attention(slot, capacity, placed, caches, lat, mass)

        @pl.when(is_kind(k, "v"))
        def _():
            first = pick(before["v"], k) * group
            for i in range(group):
                suffix_values(
                    first + i, forks, pairs, perm_ref[...], suffix_lat, suffix_mass, w_ref,
                    suffix_value, moved_mass,
                )

        return carry

    lax.fori_loop(0, len(kinds), step, 0)

    def finish(r, carry):
        for i in range(4):
            combine(4 * r + i, pairs, lat, w_ref, mass, suffix_value, moved_mass, out_ref)
        return carry

    lax.fori_loop(0, 2 * pairs // 4, finish, 0)
    exchange.finish()


def fused(queries, prefix_cache, suffix_cache, w_uv, fork_prompt, prompt_slot, suffix_len):
    forks, columns = queries.shape
    heads = w_uv.shape[0]
    pairs = heads // 2
    slots, parts = lax.axis_size("dp"), lax.axis_size("tp")
    planes = slots // 2
    rows = slots * slot_capacity(forks, slots)
    keys = prefix_cache.shape[2]
    pitch = heads + 8
    dma = pltpu.SemaphoreType.DMA
    vmem = pl.BlockSpec(memory_space=pltpu.VMEM)
    smem = pl.BlockSpec(memory_space=pltpu.SMEM)
    hbm = pl.BlockSpec(memory_space=pl.ANY)
    bf16, f32 = jnp.bfloat16, jnp.float32
    return pl.pallas_call(
        fused_kernel,
        in_specs=[smem, smem, vmem, hbm, hbm, hbm, hbm],
        out_specs=[vmem, vmem],
        out_shape=[
            jax.ShapeDtypeStruct((rows, heads * V), bf16),
            jax.ShapeDtypeStruct((rows, forks), bf16),
        ],
        scratch_shapes=[
            pltpu.VMEM((slots, parts, R + 3 * P_SIZE, keys), bf16),
            pltpu.VMEM(suffix_cache.shape, bf16),
            pltpu.VMEM((forks, columns), bf16),
            pltpu.VMEM((forks * pairs * PITCH, 128), f32),
            pltpu.VMEM((pairs, rows, PAIR), bf16),
            pltpu.VMEM(w_uv.shape, bf16),
            pltpu.VMEM((R // 128, forks * pitch, 128), f32),
            pltpu.VMEM((forks * pitch, 128), f32),
            pltpu.VMEM((heads, rows, V), bf16),
            pltpu.VMEM((heads, rows, 128), f32),
            pltpu.VMEM((heads, rows, R), bf16),
            pltpu.VMEM((heads, rows, 128), f32),
            dma((3,)),
            dma,
            dma((7, planes, 2)),
            dma((5, planes, 2)),
            dma((slots * 2,)),
            dma((slots * 2,)),
        ],
        compiler_params=pltpu.CompilerParams(
            collective_id=0, has_side_effects=True, vmem_limit_bytes=67043328
        ),
        name="fused",
    )(prompt_slot, suffix_len, fork_prompt, prefix_cache, queries, suffix_cache, w_uv)


def slot_capacity(forks, slots):
    return max(2, 2 * forks // slots)


def gather_plan(*args):
    mixed, placing = fused(*args)
    return lax.dot_general(
        placing, mixed, (((0,), (0,)), ((), ())), preferred_element_type=jnp.float32
    ).astype(jnp.bfloat16)


def shards(queries, prefix_cache, *others):
    owners_count = lax.axis_size("dp")
    forks_here = queries.shape[0]
    capacity = max(2, 2 * forks_here // owners_count)
    sent = owners_count * capacity * queries.shape[1]
    gathered = owners_count * lax.axis_size("tp") * prefix_cache.size
    square = lax.axis_size("tp") == 4 and owners_count == 2 * len(EDGE_SLOTS) // 2
    plan = gather_plan if square and gathered <= 4 * sent else exchange_plan
    return plan(queries, prefix_cache, *others)


def solution(mesh):
    placed = (
        P("dp", "tp"),
        P("dp", None, "tp"),
        P("dp", None, None),
        P("tp", None, None),
        P("dp", None),
        P(),
        P("dp"),
    )
    return jax.shard_map(
        shards, mesh=mesh, in_specs=placed, out_specs=P("dp", "tp"), check_vma=False
    )
```

```python
import functools

import jax
import jax.numpy as jnp
from jax import lax
from jax.experimental import pallas as pl
from jax.experimental.pallas import tpu as pltpu
from jax.sharding import PartitionSpec as P

R = 512
P_SIZE = 64
V = 128


score_scale = 192.0 ** (-0.5)
log2e = 1.4426950408889634
OUTER = (((1,), (1,)), ((), ()))


def project(latent, w_uv):
    return jnp.einsum("nhr,hrv->nhv", latent, w_uv, preferred_element_type=jnp.float32).astype(
        jnp.bfloat16
    )


def exchange_plan(queries, prefix_cache, suffix_cache, w_uv, fork_prompt, prompt_slot, suffix_len):
    owners_count = lax.axis_size("dp")
    forks_here = queries.shape[0]
    heads_here = w_uv.shape[0]
    key_width = R + P_SIZE
    capacity = max(2, 2 * forks_here // owners_count)
    slots_all = owners_count * capacity
    prompt_ids = jnp.arange(prompt_slot.shape[0], dtype=jnp.int32)
    chosen = fork_prompt[:, 0][:, None] == prompt_ids[None, :]
    owner_slot = jnp.sum(jnp.where(chosen, prompt_slot[None, :], 0), axis=1)
    fork_order = jnp.arange(forks_here, dtype=jnp.int32)
    before = (owner_slot[:, None] == owner_slot[None, :]) & (
        fork_order[None, :] < fork_order[:, None]
    )
    slot_rank = jnp.sum(before.astype(jnp.int32), axis=1)
    target = owner_slot * capacity + slot_rank
    placing = target[None, :] == jnp.arange(slots_all, dtype=jnp.int32)[:, None]
    outbound = jnp.dot(
        placing.astype(jnp.bfloat16), queries, preferred_element_type=jnp.float32
    ).astype(jnp.bfloat16)
    outbound = outbound.reshape(owners_count, capacity, heads_here * key_width)
    gathered = lax.all_gather(prefix_cache, "tp", axis=2, tiled=True)[0]
    received = lax.all_to_all(outbound, "dp", split_axis=0, concat_axis=0, tiled=True)
    sources = received.shape[0]
    items = received.shape[1]
    lead_rows = sources * items
    query_rows = received.reshape(lead_rows * heads_here, key_width)
    scores = jnp.dot(query_rows, gathered, preferred_element_type=jnp.float32) * score_scale
    peak_score = jnp.max(scores, axis=1, keepdims=True)
    weights = jnp.exp(scores - peak_score)
    mass_sum = jnp.sum(weights, axis=1)
    summed = lax.dot_general(
        weights.astype(jnp.bfloat16),
        gathered[:R],
        (((1,), (1,)), ((), ())),
        preferred_element_type=jnp.float32,
    )
    latent = (summed / mass_sum[:, None]).astype(jnp.bfloat16)
    log_mass = (peak_score[:, 0] + jnp.log(mass_sum)).reshape(sources, items, heads_here)
    result = project(latent.reshape(lead_rows, heads_here, R), w_uv)
    result = result.reshape(sources, items, heads_here * V)
    answer, answer_mass = (
        lax.all_to_all(result, "dp", split_axis=0, concat_axis=0, tiled=True),
        lax.all_to_all(
            log_mass.astype(jnp.bfloat16), "dp", split_axis=0, concat_axis=0, tiled=True
        ).astype(log_mass.dtype),
    )
    picking = placing.astype(jnp.bfloat16)
    flat_answer = answer.reshape(slots_all, answer.shape[2])
    returned = lax.dot_general(
        picking, flat_answer, (((0,), (0,)), ((), ())), preferred_element_type=jnp.float32
    ).astype(jnp.bfloat16)
    mass_prefix = lax.dot_general(
        placing.astype(jnp.float32),
        answer_mass.reshape(slots_all, heads_here),
        (((0,), (0,)), ((), ())),
        precision=lax.Precision.HIGHEST,
    )
    value_prefix = returned.reshape(forks_here, heads_here, V)
    query_heads = queries.reshape(forks_here, heads_here, key_width)
    suffix_scores = (
        jnp.einsum("fhe,fes->fhs", query_heads, suffix_cache, preferred_element_type=jnp.float32)
        * score_scale
    )
    positions = jnp.arange(suffix_cache.shape[2], dtype=jnp.int32)
    live_mask = (positions[None, :] < suffix_len[:, None])[:, None, :]
    suffix_scores = jnp.where(live_mask, suffix_scores, -jnp.inf)
    suffix_peak = jnp.max(suffix_scores, axis=2, keepdims=True)
    suffix_weights = jnp.where(live_mask, jnp.exp(suffix_scores - suffix_peak), 0.0)
    suffix_sum = jnp.sum(suffix_weights, axis=2)
    suffix_summed = jnp.einsum(
        "fhs,frs->fhr",
        suffix_weights.astype(jnp.bfloat16),
        suffix_cache[:, :R, :],
        preferred_element_type=jnp.float32,
    )
    latent_suffix = (suffix_summed / suffix_sum[..., None]).astype(jnp.bfloat16)
    mass_suffix = suffix_peak[..., 0] + jnp.log(suffix_sum)
    value_suffix = project(latent_suffix, w_uv)
    top_mass = jnp.maximum(mass_prefix, mass_suffix)
    share_prefix = jnp.exp(mass_prefix - top_mass)[..., None]
    share_suffix = jnp.exp(mass_suffix - top_mass)[..., None]
    combined = (
        share_prefix * value_prefix.astype(jnp.float32)
        + share_suffix * value_suffix.astype(jnp.float32)
    ) / (share_prefix + share_suffix)
    return combined.astype(jnp.bfloat16).reshape(forks_here, heads_here * V)


MESH = pl.DeviceIdType.MESH
PAIR = 2 * (R + P_SIZE)
WINDOW = R + 2 * P_SIZE
TILES = WINDOW // 128
PITCH = 2 * TILES + 1


def slot_rows(owner, slots, capacity):
    forks = owner.shape[1]
    down = lax.broadcasted_iota(jnp.int32, (forks, forks), 0)
    across = lax.broadcasted_iota(jnp.int32, (forks, forks), 1)
    wide = jnp.broadcast_to(owner, (forks, forks))
    column = jnp.sum(jnp.where(down == across, wide, 0.0), axis=1, keepdims=True)
    ahead = (column == wide) & (down < across)
    rank = jnp.sum(jnp.where(ahead, 1.0, 0.0), axis=0, keepdims=True)
    target = (owner * capacity + rank).astype(jnp.int32)
    rows = lax.broadcasted_iota(jnp.int32, (slots * capacity, forks), 0)
    return jnp.where(rows == target, 1.0, 0.0)


def stage_queries(p, q_ref, perm, staged_ref, placed_ref):
    forks = q_ref.shape[0]
    columns = pl.ds(pl.multiple_of(p * PAIR, 128), PAIR)
    pair = q_ref[:, columns].astype(jnp.float32)
    even = pair[:, :WINDOW]
    odd = pltpu.roll(pair[:, PAIR - WINDOW :], WINDOW - P_SIZE, 1)
    pairs = placed_ref.shape[1]
    for half, part in enumerate((even, odd)):
        placed_ref[half, p] = jnp.dot(
            perm, part.astype(jnp.bfloat16), preferred_element_type=jnp.float32
        ).astype(jnp.bfloat16)
        for b in range(forks // 8):
            for j in range(TILES):
                row = ((b * pairs + p) * PITCH + half * TILES + j) * 8
                staged_ref[pl.ds(pl.multiple_of(row, 8), 8), :] = part[
                    b * 8 : b * 8 + 8, j * 128 : j * 128 + 128
                ]


def suffix_chunk(first, block, pairs, lens_ref, staged_ref, cache_ref, lat_ref, mass_ref):
    heads = 2 * pairs
    pitch = heads + 8
    keys = cache_ref.shape[2]
    base = first // 8 * pairs * PITCH * 8 + first % 8
    positions = lax.broadcasted_iota(jnp.int32, (1, keys), 1)
    batch = 128 // heads
    for start in range(0, block, batch):
        masses, latents, weights = [], [], []
        for i in range(batch):
            s = start + i
            f = first + s
            halves = []
            for half in range(2):
                halves.append(
                    jnp.concatenate(
                        [
                            staged_ref[
                                pl.ds(base + (half * TILES + j) * 8 + s, pairs, stride=PITCH * 8), :
                            ]
                            for j in range(TILES)
                        ],
                        axis=1,
                    )
                )
            q = jnp.concatenate(halves, axis=0)[:, : R + P_SIZE].astype(jnp.bfloat16)
            scores = jnp.dot(q, cache_ref[f], preferred_element_type=jnp.float32)
            live = positions < lens_ref[f]
            scores = jnp.where(live, scores * (score_scale * log2e), -jnp.inf)
            peak = jnp.max(scores, axis=1, keepdims=True)
            weight = jnp.exp2(scores - peak)
            mass = jnp.sum(weight, axis=1, keepdims=True)
            rows = pl.ds(pl.multiple_of(f * pitch, 8), heads)
            mass_ref[rows, :] = jnp.broadcast_to(peak + jnp.log2(mass), (heads, 128))
            masses.append(mass)
            latents.append(cache_ref[f, :R, :])
            blocks = [jnp.zeros((heads, keys), jnp.bfloat16)] * batch
            blocks[i] = weight.astype(jnp.bfloat16)
            weights.append(jnp.concatenate(blocks, axis=0))
        summed = lax.dot_general(
            jnp.concatenate(latents, axis=1),
            jnp.concatenate(weights, axis=1),
            OUTER,
            preferred_element_type=jnp.float32,
        )
        latent = summed.T / jnp.concatenate(masses, axis=0)
        for i in range(batch):
            rows = pl.ds(pl.multiple_of((first + start + i) * pitch, 8), heads)
            for j in range(R // 128):
                lat_ref[j, rows, :] = latent[i * heads : (i + 1) * heads, j * 128 : j * 128 + 128]


def in_parts(value):
    high = value.astype(jnp.bfloat16)
    rest = value - high.astype(jnp.float32)
    mid = rest.astype(jnp.bfloat16)
    low = (rest - mid.astype(jnp.float32)).astype(jnp.bfloat16)
    return jnp.concatenate([high, mid, low], axis=0)


def head_of(r, pairs):
    return 2 * (r % pairs) + r // pairs


def suffix_values(r, forks, pairs, perm, lat_ref, mass_ref, w_ref, value_ref, moved_ref):
    pitch = 2 * pairs + 8
    rows = pl.ds(r, forks, stride=pitch)
    latent = jnp.concatenate([lat_ref[j, rows, :] for j in range(R // 128)], axis=1)
    value = jnp.dot(
        latent.astype(jnp.bfloat16), w_ref[head_of(r, pairs)], preferred_element_type=jnp.float32
    ).astype(jnp.bfloat16)
    none = jnp.zeros((2 * forks, V), jnp.bfloat16)
    both = jnp.concatenate(
        [jnp.concatenate([value, none], axis=0), in_parts(mass_ref[rows, :])], axis=1
    )
    moved = jnp.dot(perm, both, preferred_element_type=jnp.float32)
    value_ref[r] = moved[:, :V].astype(jnp.bfloat16)
    moved_ref[r] = moved[:, V:]


def slot_attention(slot, capacity, placed_ref, caches_ref, lat_ref, mass_ref):
    pairs = placed_ref.shape[1]
    parts = caches_ref.shape[1]
    own = pl.ds(pl.multiple_of(slot * capacity, capacity), capacity)
    q = jnp.concatenate(
        [placed_ref[half, p, own, :] for half in range(2) for p in range(pairs)], axis=0
    )
    scores = [
        jnp.dot(q, caches_ref[slot, k], preferred_element_type=jnp.float32) for k in range(parts)
    ]
    peak = functools.reduce(
        jnp.maximum, [jnp.max(piece, axis=1, keepdims=True) for piece in scores]
    )
    mass = 0.0
    summed = 0.0
    for k in range(parts):
        weight = jnp.exp2((scores[k] - peak) * (score_scale * log2e))
        mass = mass + jnp.sum(weight, axis=1, keepdims=True)
        summed = summed + lax.dot_general(
            weight.astype(jnp.bfloat16),
            caches_ref[slot, k, :R, :],
            OUTER,
            preferred_element_type=jnp.float32,
        )
    latent = (summed / mass).astype(jnp.bfloat16)
    lat_ref[:, own, :] = latent.reshape(2 * pairs, capacity, R)
    log_mass = peak * (score_scale * log2e) + jnp.log2(mass)
    mass_ref[:, own, :] = jnp.broadcast_to(log_mass, (log_mass.shape[0], 128)).reshape(
        2 * pairs, capacity, 128
    )


def combine(r, pairs, lat_ref, w_ref, mass_ref, value_ref, moved_ref, out_ref):
    h = head_of(r, pairs)
    value = jnp.dot(lat_ref[r], w_ref[h], preferred_element_type=jnp.float32)
    value = value.astype(jnp.bfloat16).astype(jnp.float32)
    ours, theirs = mass_ref[r], moved_ref[r]
    top = jnp.maximum(ours, theirs)
    ours = jnp.exp2(ours - top)
    theirs = jnp.exp2(theirs - top)
    mixed = (ours * value + theirs * value_ref[r].astype(jnp.float32)) / (ours + theirs)
    out_ref[:, pl.ds(pl.multiple_of(h * 128, 128), 128)] = mixed.astype(jnp.bfloat16)


class Exchange:
    def __init__(self, caches, own, own_sem, sems):
        dp, tp = lax.axis_index("dp"), lax.axis_index("tp")
        self.planes = caches.shape[0] // 2
        self.z, self.x = dp // 2, dp % 2
        self.y, self.c = tp // 2, tp % 2
        self.caches, self.own, self.own_sem = caches, own, own_sem
        self.sems = sems
        self.low = self.z < self.planes // 2
        inward = jnp.where(self.low, self.z + 1, self.z - 1)
        outward = jnp.clip(jnp.where(self.low, self.z - 1, self.z + 1), 0, self.planes - 1)
        self.edge = (self.z == 0) | (self.z == self.planes - 1)
        self.to = dict(
            x=(self.z * 2 + 1 - self.x, tp),
            y=(dp, (1 - self.y) * 2 + self.c),
            pair=(dp, self.y * 2 + 1 - self.c),
            inward=(inward * 2 + self.x, tp),
            outward=(outward * 2 + self.x, tp),
        )
        self.rows = own.shape[1]

    def plane(self, q):
        return jnp.where(self.low, q, self.planes - 1 - q)

    def place(self, q, far_x=0, far_y=0, half=None):
        xx = 1 - self.x if far_x else self.x
        yy = 1 - self.y if far_y else self.y
        first, count = 0, self.rows
        if half is not None:
            count = self.rows // 2
            first = half * count
        return self.caches.at[self.plane(q) * 2 + xx, yy * 2 + self.c, pl.ds(first, count)]

    def copy(self, kind, q, half, sender):
        far_x, far_y, index = {
            "u": (0, 0, 0),
            "d": (1, 1, 1),
            "x": (0, 0, 2),
            "y": (0, 0, 3),
            "dx": (0, 1, 4),
            "dy": (1, 0, 4),
        }[kind]
        link = {"x": "x", "dx": "x", "y": "y", "dy": "y"}.get(kind, sender)
        sends = {"inward": 0, "outward": 2, "x": 4, "y": 5, "dx": 6, "dy": 6}
        send = sends[sender] + (kind == "d") if kind in ("u", "d") else sends[kind]
        part = self.place(q, far_x, far_y, half)
        zz = self.plane(q)
        send_sem, recv_sem = self.sems["send"], self.sems["recv"]
        return pltpu.make_async_remote_copy(
            src_ref=part,
            dst_ref=part,
            send_sem=send_sem.at[send, zz, half],
            recv_sem=recv_sem.at[index, zz, half],
            device_id=self.to[link],
            device_id_type=MESH,
        )

    def send(self, kind, q, half, sender=None):
        self.copy(kind, q, half, sender).start()
        self.sent.append((kind, q, half, sender))

    def got(self, kind, q, half):
        self.copy(kind, q, half, "inward").wait_recv()

    def pair(self, q, far_x, far_y):
        part = self.place(q, far_x, far_y)
        xx = 1 - self.x if far_x else self.x
        yy = 1 - self.y if far_y else self.y
        k = (self.plane(q) * 2 + xx) * 2 + yy
        return pltpu.make_async_remote_copy(
            src_ref=part,
            dst_ref=part,
            send_sem=self.sems["pair_send"].at[k],
            recv_sem=self.sems["pair_recv"].at[k],
            device_id=self.to["pair"],
            device_id_type=MESH,
        )

    def load(self):
        return pltpu.make_async_copy(self.own.at[0], self.place_own(), self.own_sem)

    def place_own(self):
        slot = self.z * 2 + self.x
        return self.caches.at[slot, self.y * 2 + self.c, pl.ds(0, self.rows)]

    def barrier(self):
        sem = pltpu.get_barrier_semaphore()
        for name in ("x", "y", "pair", "inward"):
            pl.semaphore_signal(sem, inc=1, device_id=self.to[name], device_id_type=MESH)

        @pl.when(~self.edge)
        def _():
            pl.semaphore_signal(sem, inc=1, device_id=self.to["outward"], device_id_type=MESH)

        pl.semaphore_wait(sem, jnp.where(self.edge, 4, 5))

    def rounds(self, edge):
        send, got = self.send, self.got
        self.sent = []

        def first():
            q = 0 if edge else 1
            for half in range(2):
                send("u", q, half, "inward")
                if not edge:
                    send("u", q, half, "outward")
                send("x", q, half)
                send("y", q, 1 - half)
            self.pair(q, 0, 0).start()

        def both(kind, q):
            got(kind, q, 0)
            got(kind, q, 1)

        def sides(q):
            both("x", q)
            self.pair(q, 1, 0).start()
            both("y", q)
            self.pair(q, 0, 1).start()

        def sides_late(q):
            got("x", q, 1)
            self.pair(q, 1, 0).start()
            got("y", q, 0)
            self.pair(q, 0, 1).start()

        def cross(q):
            got("x", q, 0)
            send("dy", q, 0)
            got("y", q, 1)
            send("dx", q, 1)

        def crossed(q):
            got("dy", q, 0)
            got("dx", q, 1)
            self.pair(q, 1, 1).start()

        def diagonal(q):
            both("d", q)
            self.pair(q, 1, 1).start()

        def e1():
            cross(0)
            got("u", 1, 0)
            send("x", 1, 0)
            send("y", 1, 0)

        def e2():
            got("u", 1, 1)
            send("x", 1, 1)
            send("y", 1, 1)
            self.pair(1, 0, 0).start()
            sides_late(0)

        def e3():
            crossed(0)
            got("u", 2, 0)
            send("x", 2, 0)
            send("y", 2, 0)

        def e4():
            got("u", 2, 1)
            send("x", 2, 1)
            send("y", 2, 1)
            self.pair(2, 0, 0).start()

        def e5():
            sides(1)
            got("u", 3, 0)
            send("x", 3, 0)

        def e6():
            got("u", 3, 1)
            send("y", 3, 1)
            send("y", 3, 0)
            send("x", 3, 1)
            self.pair(3, 0, 0).start()

        def e7():
            sides(2)

        def e8():
            cross(3)
            diagonal(1)

        def e9():
            sides_late(3)

        def e10():
            crossed(3)
            diagonal(2)

        def i1():
            cross(1)
            got("u", 2, 0)
            send("u", 2, 0, "outward")
            got("u", 0, 0)
            send("u", 0, 0, "inward")
            send("x", 0, 0)

        def i2():
            got("u", 2, 1)
            send("u", 2, 1, "outward")
            got("u", 0, 1)
            send("u", 0, 1, "inward")
            send("y", 0, 1)
            send("y", 0, 0)
            send("x", 0, 1)
            self.pair(2, 0, 0).start()
            self.pair(0, 0, 0).start()
            sides_late(1)

        def i3():
            crossed(1)
            for half in range(2):
                send("d", 1, half, "inward")
            got("u", 3, 0)
            send("u", 3, 0, "outward")

        def i4():
            got("u", 3, 1)
            send("u", 3, 1, "outward")
            self.pair(3, 0, 0).start()
            for half in range(2):
                send("d", 1, half, "outward")
            cross(0)
            for q in (2, 3):
                for half in range(2):
                    send("x", q, half)
                    send("y", q, half)

        def i5():
            sides_late(0)

        def i6():
            crossed(0)
            for half in range(2):
                send("d", 0, half, "inward")
            for half in range(2):
                got("d", 2, half)
                send("d", 2, half, "outward")
            self.pair(2, 1, 1).start()

        def i7():
            pass

        def i8():
            sides(2)

        def i9():
            diagonal(3)

        def i10():
            sides(3)

        if edge:
            return [first, e1, e2, e3, e4, e5, e6, e7, e8, e9, e10]
        return [first, i1, i2, i3, i4, i5, i6, i7, i8, i9, i10]

    def round(self, r):
        edge = []
        for side, when in ((True, self.edge), (False, ~self.edge)):
            @pl.when(when)
            def _(side=side):
                self.rounds(side)[r]()
            edge.append(self.sent)
        self.all_sent = getattr(self, "all_sent", [])
        self.all_sent.append(edge)

    def finish(self):
        for side, when in ((0, self.edge), (1, ~self.edge)):
            @pl.when(when)
            def _(side=side):
                for sent in self.all_sent:
                    for item in sent[side]:
                        self.copy(*item).wait_send()
        for k in range(2 * self.caches.shape[0]):
            pltpu.make_async_remote_copy(
                src_ref=self.place_own(), dst_ref=self.place_own(),
                send_sem=self.sems["pair_send"].at[k], recv_sem=self.sems["pair_recv"].at[k],
                device_id=self.to["pair"], device_id_type=MESH).wait_send()

    def pair_done(self, slot, y):
        pltpu.make_async_remote_copy(
            src_ref=self.place_own(), dst_ref=self.place_own(),
            send_sem=self.sems["pair_send"].at[slot * 2 + y], recv_sem=self.sems["pair_recv"].at[slot * 2 + y],
            device_id=self.to["pair"], device_id_type=MESH).wait_recv()


def pick(table, index):
    value = table[-1]
    for i in range(len(table) - 2, -1, -1):
        value = jnp.where(index == i, table[i], value)
    return value


EDGE_SLOTS = ((0, 0), (0, 1), (1, 0), (2, 0), (1, 1), (3, 0), (2, 1), (3, 1))
INNER_SLOTS = ((1, 0), (1, 1), (0, 0), (0, 1), (2, 0), (2, 1), (3, 0), (3, 1))
PLAN = ("h", "hhh", "hhh", "ah", "avv", "vvva", "vvv", "a", "a", "a", "aa")


def fused_kernel(
    slot_ref,
    lens_ref,
    prompt_ref,
    own,
    q_hbm,
    suffix_hbm,
    w_hbm,
    out_ref,
    mixed_ref,
    perm_ref,
    caches,
    held,
    q_ref,
    staged,
    placed,
    w_ref,
    suffix_lat,
    suffix_mass,
    suffix_value,
    moved_mass,
    lat,
    mass,
    load_sems,
    own_sem,
    send_sems,
    recv_sems,
    pair_send,
    pair_recv,
):
    forks = q_ref.shape[0]
    pairs = placed.shape[1]
    slots = caches.shape[0]
    capacity = placed.shape[2] // slots
    exchange = Exchange(
        caches,
        own,
        own_sem,
        dict(send=send_sems, recv=recv_sems, pair_send=pair_send, pair_recv=pair_recv),
    )
    exchange.load().start()
    sources = ((q_hbm, q_ref), (suffix_hbm, held), (w_hbm, w_ref))
    loads = [pltpu.make_async_copy(a, b, load_sems.at[i]) for i, (a, b) in enumerate(sources)]
    loads[0].start()
    exchange.barrier()
    exchange.load().wait()
    exchange.round(0)
    loads[1].start()
    loads[2].start()

    pad = jnp.zeros((caches.shape[1], P_SIZE, caches.shape[3]), jnp.bfloat16)

    def clear(s, carry):
        caches[s, :, R + P_SIZE :, :] = pad
        return carry

    lax.fori_loop(0, slots, clear, 0)
    owner = jnp.zeros(prompt_ref.shape, jnp.float32)
    for p in range(slot_ref.shape[0]):
        owner = jnp.where(prompt_ref[...] == p, slot_ref[p].astype(jnp.float32), owner)
    perm_ref[...] = slot_rows(owner, slots, capacity).astype(jnp.bfloat16)
    loads[0].wait()

    def stage(p, carry):
        stage_queries(p, q_ref, perm_ref[...], staged, placed)
        return carry

    lax.fori_loop(0, pairs, stage, 0)
    loads[1].wait()
    loads[2].wait()

    kinds = "".join(PLAN)
    count = {kind: kinds.count(kind) for kind in "hav"}
    before = {
        kind: [kinds[:k].count(kind) for k in range(len(kinds))] for kind in "hav"
    }
    starts = [sum(len(part) for part in PLAN[:r]) for r in range(len(PLAN))]
    block = forks // count["h"]
    group = 2 * pairs // count["v"]

    def is_kind(k, kind):
        hit = k < 0
        for i, name in enumerate(kinds):
            if name == kind:
                hit = hit | (k == i)
        return hit

    def step(k, carry):
        for r in range(1, len(PLAN)):
            @pl.when(k == starts[r])
            def _(r=r):
                exchange.round(r)

        @pl.when(is_kind(k, "h"))
        def _():
            first = pick(before["h"], k) * block
            suffix_chunk(first, block, pairs, lens_ref, staged, held, suffix_lat, suffix_mass)

        @pl.when(is_kind(k, "a"))
        def _():
            n = pick(before["a"], k)
            q = jnp.where(
                exchange.edge, pick([s[0] for s in EDGE_SLOTS], n), pick([s[0] for s in INNER_SLOTS], n)
            )
            far = jnp.where(
                exchange.edge, pick([s[1] for s in EDGE_SLOTS], n), pick([s[1] for s in INNER_SLOTS], n)
            )
            xx = jnp.where(far == 1, 1 - exchange.x, exchange.x)
            slot = exchange.plane(q) * 2 + xx
            exchange.pair_done(slot, 0)
            exchange.pair_done(slot, 1)
            slot_attention(slot, capacity, placed, caches, lat, mass)

        @pl.when(is_kind(k, "v"))
        def _():
            first = pick(before["v"], k) * group
            perm = perm_ref[...]
            perm = jnp.concatenate([perm, perm, perm], axis=1)
            for i in range(group):
                suffix_values(
                    first + i, forks, pairs, perm, suffix_lat, suffix_mass, w_ref,
                    suffix_value, moved_mass,
                )

        return carry

    lax.fori_loop(0, len(kinds), step, 0)

    def finish(r, carry):
        for i in range(8):
            combine(8 * r + i, pairs, lat, w_ref, mass, suffix_value, moved_mass, mixed_ref)
        return carry

    lax.fori_loop(0, 2 * pairs // 8, finish, 0)
    perm = perm_ref[...]
    for j in range(0, out_ref.shape[1], 256):
        out_ref[:, j : j + 256] = lax.dot_general(
            perm, mixed_ref[:, j : j + 256], (((0,), (0,)), ((), ())), preferred_element_type=jnp.float32
        ).astype(jnp.bfloat16)
    exchange.finish()


def fused(queries, prefix_cache, suffix_cache, w_uv, fork_prompt, prompt_slot, suffix_len):
    forks, columns = queries.shape
    heads = w_uv.shape[0]
    pairs = heads // 2
    slots, parts = lax.axis_size("dp"), lax.axis_size("tp")
    planes = slots // 2
    rows = slots * slot_capacity(forks, slots)
    keys = prefix_cache.shape[2]
    pitch = heads + 8
    dma = pltpu.SemaphoreType.DMA
    vmem = pl.BlockSpec(memory_space=pltpu.VMEM)
    smem = pl.BlockSpec(memory_space=pltpu.SMEM)
    hbm = pl.BlockSpec(memory_space=pl.ANY)
    bf16, f32 = jnp.bfloat16, jnp.float32
    return pl.pallas_call(
        fused_kernel,
        in_specs=[smem, smem, vmem, hbm, hbm, hbm, hbm],
        out_specs=vmem,
        out_shape=jax.ShapeDtypeStruct((forks, heads * V), bf16),
        scratch_shapes=[
            pltpu.VMEM((rows, heads * V), bf16),
            pltpu.VMEM((rows, forks), bf16),
            pltpu.VMEM((slots, parts, WINDOW, keys), bf16),
            pltpu.VMEM(suffix_cache.shape, bf16),
            pltpu.VMEM((forks, columns), bf16),
            pltpu.VMEM((forks * pairs * PITCH, 128), f32),
            pltpu.VMEM((2, pairs, rows, WINDOW), bf16),
            pltpu.VMEM(w_uv.shape, bf16),
            pltpu.VMEM((R // 128, forks * pitch, 128), f32),
            pltpu.VMEM((forks * pitch, 128), f32),
            pltpu.VMEM((heads, rows, V), bf16),
            pltpu.VMEM((heads, rows, 128), f32),
            pltpu.VMEM((heads, rows, R), bf16),
            pltpu.VMEM((heads, rows, 128), f32),
            dma((3,)),
            dma,
            dma((7, planes, 2)),
            dma((5, planes, 2)),
            dma((slots * 2,)),
            dma((slots * 2,)),
        ],
        compiler_params=pltpu.CompilerParams(
            collective_id=0, has_side_effects=True, vmem_limit_bytes=67043328
        ),
        name="fused",
    )(prompt_slot, suffix_len, fork_prompt.reshape(1, forks), prefix_cache, queries, suffix_cache, w_uv)


def slot_capacity(forks, slots):
    return max(2, 2 * forks // slots)


def gather_plan(*args):
    return fused(*args)


def shards(queries, prefix_cache, *others):
    owners_count = lax.axis_size("dp")
    forks_here = queries.shape[0]
    capacity = max(2, 2 * forks_here // owners_count)
    sent = owners_count * capacity * queries.shape[1]
    gathered = owners_count * lax.axis_size("tp") * prefix_cache.size
    square = lax.axis_size("tp") == 4 and owners_count == 2 * len(EDGE_SLOTS) // 2
    plan = gather_plan if square and gathered <= 4 * sent else exchange_plan
    return plan(queries, prefix_cache, *others)


def solution(mesh):
    placed = (
        P("dp", "tp"),
        P("dp", None, "tp"),
        P("dp", None, None),
        P("tp", None, None),
        P("dp", None),
        P(),
        P("dp"),
    )
    return jax.shard_map(
        shards, mesh=mesh, in_specs=placed, out_specs=P("dp", "tp"), check_vma=False
    )
```
